32 devices in a mesh: gx: 4 (over y, x), gy: 2 (over core), gz: 4 (over z).
Axes of the slice: x: 2, y: 2, z: 4, core: 2. Of those that a mesh axis runs over, the one named last changes fastest.
Arguments:
- spectrum: float32 [3, 2, 16, 16, 2048], P(None, None, ('gy', 'gx'), None, 'gz'), may hold values from -0.3125 to 0.3125
- theta: float32 [16, 16, 8192], P('gy', 'gz', 'gx'), may hold values from -6 to 6
- section_sum: float32 [16, 16, 8192], P('gy', 'gz', 'gx'), may hold values from -6 to 6
- seg_offset: int32 [4], replicated, may hold values from 0 to 2560, as said below
- seg_length: int32 [4], replicated, may hold values from 512 to 1536, as said below
- stencil_index: int32 [8, 8192], replicated, may hold values from 0 to 1535, as said below
- stencil_weight: float32 [8, 8192], replicated, may hold values from 0 to 0.25
Outputs:
- theta_next: float32 [16, 16, 8192], P('gy', 'gz', 'gx')
- section_next: float32 [16, 16, 8192], P('gy', 'gz', 'gx')
The draws below stay inside these ranges and needn't reach their ends.
Inputs may be any that keep to these rules, and one draw needn't show every extreme that they name: `seg_length`: some block's segment holds exactly 1536 cells. For every block i, seg_offset[i] + 1536 <= 4096. `stencil_index`: positions count from the start of the segment of the scalar cell's x block; taps at or past that segment's length are padding.
All inputs are finite; a program needn't handle non-finite values.
Results may differ from the reference program's by a relative error of at most 0.00005.
Values sent between devices are 32-bit elements; how exact they have to be, the bound alone decides.
A program may use at most 64 MiB of HBM per device.

```python
import jax
import jax.numpy as jnp
from jax import lax

TAPS = 8
NVX = 4096
K = 2048
NSX = 8192
NSY = 16
NSZ = 16
MAXSEG = 1536
N_GX = 4


def segments_drawn(key):
    base_key = jax.random.fold_in(key, 7)
    length_key, longest_key = jax.random.split(base_key)
    lengths = jax.random.randint(length_key, (N_GX,), MAXSEG // 3, MAXSEG + 1, dtype=jnp.int32)
    longest = jax.random.randint(longest_key, (), 0, N_GX, dtype=jnp.int32)
    block_number = jnp.arange(N_GX, dtype=jnp.int32)
    lengths = jnp.where(block_number == longest, MAXSEG, lengths)
    centers = block_number * (NVX // N_GX) + NVX // (2 * N_GX)
    offsets = jnp.clip(centers - lengths // 2, 0, NVX - MAXSEG)
    return (offsets.astype(jnp.int32), lengths.astype(jnp.int32))


def draw_seg_offset(key, part):
    return segments_drawn(key)[0]


def draw_seg_length(key, part):
    return segments_drawn(key)[1]


def draw_stencil_index(key, part):
    offsets, lengths = segments_drawn(key)
    block_cells = NSX // N_GX
    cell_index = jnp.arange(NSX, dtype=jnp.int32)
    within = cell_index % block_cells
    owner_block = cell_index // block_cells
    owner_length = jnp.sum(jnp.where(owner_block[:, None] == jnp.arange(N_GX, dtype=jnp.int32)[None, :], lengths[None, :], 0), axis=1)
    jitter = jax.random.randint(jax.random.fold_in(key, 13), (NSX,), 0, 3, dtype=jnp.int32)
    anchor = within * owner_length // block_cells + jitter
    tap_shift = jnp.arange(TAPS, dtype=jnp.int32)[:, None] - TAPS // 2 + 1
    return jnp.clip(anchor[None, :] + tap_shift, 0, MAXSEG - 1).astype(jnp.int32)


def level_of(rng, extent, shards, least, top_value):
    def one(position, shards_of):
        heights = jax.random.uniform(jax.random.fold_in(jax.random.fold_in(rng, 6), position), (shards_of,), jnp.float32, least / len(shards), top_value / len(shards))
        return jnp.repeat(jnp.exp(heights), extent[position] // shards_of).reshape((-1,) + (1,) * (len(extent) - position - 1))

    factor_of = one(*shards[0])
    for cut in shards[1:]:
        factor_of = factor_of * one(*cut)
    return factor_of


def scatter_about(rng, extent, spread, most, cuts=(), kind=jnp.bfloat16):
    entries = jax.random.normal(rng, extent, jnp.float32) * spread
    if len(cuts) > 0:
        entries = level_of(rng, extent, cuts, -0.22, 0.18) * entries
    return jnp.clip(entries, min=-most, max=most).astype(kind)


def setup_inputs(seed: int = 0) -> dict:
    seeds = jax.random.split(jax.random.key(seed), 8)
    return {
        "spectrum": scatter_about(seeds[0], (3, 2, NSY, NSZ, K), ((2.0 / NVX) ** 0.5), 0.3125, ((2, 8), (4, 4)), jnp.float32),
        "theta": scatter_about(seeds[1], (NSY, NSZ, NSX), 1.0, 6.0, ((0, 2), (1, 4), (2, 4)), jnp.float32),
        "section_sum": scatter_about(seeds[2], (NSY, NSZ, NSX), 0.5, 6.0, ((0, 2), (1, 4), (2, 4)), jnp.float32),
        "seg_offset": draw_seg_offset(jax.random.fold_in(seeds[7], 71), 0),
        "seg_length": draw_seg_length(jax.random.fold_in(seeds[7], 71), 0),
        "stencil_index": draw_stencil_index(jax.random.fold_in(seeds[7], 71), 0),
        "stencil_weight": jnp.clip(jax.random.uniform(seeds[6], (TAPS, NSX), jnp.float32, 0.0, 0.25), 0.0, 0.25),
    }


first_coeffs = (0.8, -0.2, 4.0 / 105.0, -1.0 / 280.0)
second_coeffs = (1.6, -0.2, 8.0 / 315.0, -1.0 / 560.0)
center_coeff = -205.0 / 72.0
diffusivity = 0.15
time_step = 0.4
section_keep = -5.0 / 9.0
section_gain = 15.0 / 16.0


def reference(spectrum, theta, section_sum, seg_offset, seg_length, stencil_index, stencil_weight):
    line_length = 2 * spectrum.shape[-1]
    scalar_cells = theta.shape[2]
    block_cells = scalar_cells // N_GX
    block_of = (jnp.arange(scalar_cells, dtype=jnp.int32) // block_cells).astype(jnp.int32)
    start_of = seg_offset[block_of]
    length_of = seg_length[block_of]
    absolute = (start_of[None, :] + stencil_index).astype(jnp.int32)
    live_weight = jnp.where(stencil_index < length_of[None, :], stencil_weight, 0.0)
    theta_cycle = jnp.concatenate([theta[-4:], theta, theta[:4]], axis=0)

    def one_row(row_index):
        coeffs = spectrum[:, 0, row_index] + 1j * spectrum[:, 1, row_index]
        velocity = line_length * jnp.real(jnp.fft.ifft(coeffs, n=line_length, axis=-1))
        carried = jnp.zeros((3, theta.shape[1], scalar_cells), jnp.float32)
        for tap_number in range(stencil_index.shape[0]):
            carried = carried + live_weight[tap_number] * jnp.take(velocity, absolute[tap_number], axis=-1)
        slab = lax.dynamic_slice_in_dim(theta_cycle, row_index, 9, 0)
        center = slab[4]
        grad_x = jnp.zeros_like(center)
        grad_y = jnp.zeros_like(center)
        grad_z = jnp.zeros_like(center)
        laplace = 3.0 * center_coeff * center
        for reach in range(1, 5):
            ahead_x = jnp.roll(center, -reach, axis=1)
            behind_x = jnp.roll(center, reach, axis=1)
            ahead_z = jnp.roll(center, -reach, axis=0)
            behind_z = jnp.roll(center, reach, axis=0)
            ahead_y = slab[4 + reach]
            behind_y = slab[4 - reach]
            first = first_coeffs[reach - 1]
            second = second_coeffs[reach - 1]
            grad_x = grad_x + first * (ahead_x - behind_x)
            grad_y = grad_y + first * (ahead_y - behind_y)
            grad_z = grad_z + first * (ahead_z - behind_z)
            laplace = laplace + second * (ahead_x + behind_x + ahead_y + behind_y + ahead_z + behind_z)
        change = -(carried[0] * grad_x + carried[1] * grad_y + carried[2] * grad_z) + diffusivity * laplace
        register = lax.dynamic_index_in_dim(section_sum, row_index, 0, keepdims=False)
        section_next = section_keep * register + time_step * change
        return center + section_gain * section_next, section_next

    theta_next, section_next = lax.map(one_row, jnp.arange(theta.shape[0], dtype=jnp.int32))
    return theta_next, section_next
```

```python
import functools
import math

import jax
import jax.numpy as jnp
import numpy as np
from jax import lax
from jax.experimental import pallas as pl
from jax.experimental.pallas import tpu as pltpu
from jax.sharding import PartitionSpec as P

MESH = pl.DeviceIdType.MESH
VMEM = pltpu.VMEM
LANES = 128
HALO = 4

first_coeffs = (0.8, -0.2, 4.0 / 105.0, -1.0 / 280.0)
second_coeffs = (1.6, -0.2, 8.0 / 315.0, -1.0 / 560.0)
center_coeff = -205.0 / 72.0
diffusivity = 0.15
time_step = 0.4
section_keep = -5.0 / 9.0
section_gain = 15.0 / 16.0


def whole_vmem(count):
    return [pl.BlockSpec(memory_space=VMEM)] * count


def modes_kernel(peers, spec_ref, out_ref, send, send_sem, recv_sem, own_sem):
    me = lax.axis_index("gz")
    barrier = pltpu.get_barrier_semaphore()
    for step in range(1, peers):
        pl.semaphore_signal(
            barrier, inc=1, device_id={"gz": lax.rem(me + step, peers)}, device_id_type=MESH
        )
    _, _, rows, depth, modes = spec_ref.shape
    mine = depth // peers
    lines = 3 * rows * mine
    for peer in range(peers):
        for slab in range(modes // LANES):
            for part in range(2):
                for comp in range(3):
                    for row in range(rows):
                        at = part * lines + (comp * rows + row) * mine
                        send[peer, slab, at : at + mine, :] = spec_ref[
                            comp,
                            part,
                            row,
                            peer * mine : (peer + 1) * mine,
                            slab * LANES : (slab + 1) * LANES,
                        ]
    pl.semaphore_wait(barrier, peers - 1)
    copies = []
    for step in range(1, peers):
        target = lax.rem(me + step, peers)
        copy = pltpu.make_async_remote_copy(
            src_ref=send.at[target],
            dst_ref=out_ref.at[me],
            send_sem=send_sem.at[step - 1],
            recv_sem=recv_sem.at[step - 1],
            device_id={"gz": target},
            device_id_type=MESH,
        )
        copy.start()
        copies.append(copy)
    own = pltpu.make_async_copy(send.at[me], out_ref.at[me], own_sem)
    own.start()
    own.wait()
    for copy in copies:
        copy.wait()


def exchange_modes(spectrum):
    peers = lax.axis_size("gz")
    _, _, rows, depth, modes = spectrum.shape
    shape = (peers, modes // LANES, 6 * rows * (depth // peers), LANES)
    return pl.pallas_call(
        functools.partial(modes_kernel, peers),
        out_shape=jax.ShapeDtypeStruct(shape, jnp.float32),
        in_specs=whole_vmem(1),
        out_specs=pl.BlockSpec(memory_space=VMEM),
        scratch_shapes=[
            VMEM(shape, jnp.float32),
            pltpu.SemaphoreType.DMA((peers - 1,)),
            pltpu.SemaphoreType.DMA((peers - 1,)),
            pltpu.SemaphoreType.DMA,
        ],
        compiler_params=pltpu.CompilerParams(collective_id=0, has_side_effects=True),
        name="modes",
    )(spectrum)


def rotate(value, turn):
    re, im = value
    cosine, sine = math.cos(2 * math.pi * turn), math.sin(2 * math.pi * turn)
    quarter = turn * 4 % 4
    if quarter == 0:
        return re, im
    if quarter == 1:
        return -im, re
    if quarter == 2:
        return -re, -im
    if quarter == 3:
        return im, -re
    return re * cosine - im * sine, re * sine + im * cosine


def fft(values):
    count = len(values)
    if count == 1:
        return values
    even = fft(values[0::2])
    odd = fft(values[1::2])
    low, high = [], []
    for x in range(count // 2):
        re, im = rotate(odd[x], x / count)
        low.append((even[x][0] + re, even[x][1] + im))
        high.append((even[x][0] - re, even[x][1] - im))
    return low + high


def split(value):
    top = value.astype(jnp.bfloat16)
    return top, (value - top.astype(jnp.float32)).astype(jnp.bfloat16)


def lines_kernel(offset_ref, spec_ref, twist_ref, last_ref, out_ref, mixed, velocity):
    slabs, both, _ = spec_ref.shape
    lines = both // 2
    near = 2 * slabs
    group = lines // 3
    for comp in range(3):
        re_rows = slice(comp * group, (comp + 1) * group)
        im_rows = slice(lines + comp * group, lines + (comp + 1) * group)
        values = [(spec_ref[k, re_rows, :], spec_ref[k, im_rows, :]) for k in range(slabs)]
        even = fft(values)
        for x in range(slabs):
            mixed[2 * x, re_rows, :] = even[x][0]
            mixed[2 * x, im_rows, :] = even[x][1]
        values = [(spec_ref[k, re_rows, :], spec_ref[k, im_rows, :]) for k in range(slabs)]
        odd = fft([rotate(values[k], k / near) for k in range(slabs)])
        for x in range(slabs):
            mixed[2 * x + 1, re_rows, :] = odd[x][0]
            mixed[2 * x + 1, im_rows, :] = odd[x][1]
    last_both = last_ref[...]
    far = last_both.shape[0] // 2
    last_top = last_both[:far]
    dims = (((1,), (1,)), ((), ()))

    def twisted(line):
        re, im = mixed[:, line, :], mixed[:, lines + line, :]
        pieces = []
        for quarter in range(LANES // near):
            rows = slice(quarter * near, (quarter + 1) * near)
            cosine, sine = twist_ref[0, rows, :], twist_ref[1, rows, :]
            pieces.append(jnp.concatenate([re * cosine - im * sine, re * sine + im * cosine], axis=1))
        return jnp.concatenate(pieces, axis=0)

    for pair in range(lines // 2):
        turned = jnp.concatenate([twisted(2 * pair), twisted(2 * pair + 1)], axis=0)
        top, rest = split(turned)
        first = lax.dot_general(last_both, top, dims, preferred_element_type=jnp.float32)
        second = lax.dot_general(last_top, rest, dims, preferred_element_type=jnp.float32)
        total = first[:far] + (first[far:] + second)
        velocity[:, 2 * pair, :] = total[:, :LANES]
        velocity[:, 2 * pair + 1, :] = total[:, LANES:]
    blocks, span = out_ref.shape[:2]
    for block in range(blocks):
        start = jnp.minimum(offset_ref[block] // LANES, far - span)
        out_ref[block] = velocity[pl.ds(start, span)]


def transform_lines(seg_offset, modes):
    blocks = seg_offset.shape[0]
    slabs, both, _ = modes.shape
    lines = both // 2
    length = 2 * slabs * LANES
    far = length // LANES
    span = min(3 * length // (2 * blocks) // LANES + 1, far)
    k = np.arange(LANES)
    turn = 2 * np.pi * (np.outer(k, k) % length) / length
    twist = np.stack([np.cos(turn), np.sin(turn)]).astype(np.float32)
    turn = 2 * np.pi * (np.outer(np.arange(far), k) % far) / far
    last = np.concatenate([np.cos(turn), -np.sin(turn)], axis=1).astype(np.float32)
    top = last.astype(jnp.bfloat16)
    rest = (last - top.astype(np.float32)).astype(jnp.bfloat16)
    return pl.pallas_call(
        lines_kernel,
        out_shape=jax.ShapeDtypeStruct((blocks, span, lines, LANES), jnp.float32),
        in_specs=[pl.BlockSpec(memory_space=pltpu.SMEM)] + whole_vmem(3),
        out_specs=pl.BlockSpec(memory_space=VMEM),
        scratch_shapes=[
            VMEM((2 * slabs, both, LANES), jnp.float32),
            VMEM((far, lines, LANES), jnp.float32),
        ],
        name="lines",
    )(seg_offset, modes, jnp.asarray(twist), jnp.asarray(np.concatenate([top, rest], axis=0)))


def faces_kernel(sizes, seg_ref, theta_ref, *refs):
    out_ref, halos = refs[0], refs[1:7]
    send_sem, recv_sem, own_sem = refs[7:]
    gx, gy, gz = sizes
    me = lax.axis_index("gx")
    rows, depth, cells = theta_ref.shape
    barrier = pltpu.get_barrier_semaphore()
    targets = [{"gx": lax.rem(me + step, gx)} for step in range(1, gx)]
    for axis, count in (("gy", gy), ("gz", gz)):
        here = lax.axis_index(axis)
        targets.append({axis: lax.rem(here + 1, count)})
        targets.append({axis: lax.rem(here + count - 1, count)})
    for target in targets:
        pl.semaphore_signal(barrier, inc=1, device_id=target, device_id_type=MESH)
    pl.semaphore_wait(barrier, len(targets))
    sends = []
    for step in range(1, gx):
        target = lax.rem(me + step, gx)
        sends.append((seg_ref.at[target], out_ref.at[me], {"gx": target}))
    ahead = {
        axis: {axis: lax.rem(lax.axis_index(axis) + 1, count)}
        for axis, count in (("gx", gx), ("gy", gy), ("gz", gz))
    }
    behind = {
        axis: {axis: lax.rem(lax.axis_index(axis) + count - 1, count)}
        for axis, count in (("gx", gx), ("gy", gy), ("gz", gz))
    }
    x_back, x_front, y_back, y_front, z_back, z_front = halos
    sends += [
        (theta_ref.at[:, pl.ds(depth - HALO, HALO), :], z_back, ahead["gz"]),
        (theta_ref.at[:, pl.ds(0, HALO), :], z_front, behind["gz"]),
        (theta_ref.at[:, :, pl.ds(cells - LANES, LANES)], x_back, ahead["gx"]),
        (theta_ref.at[:, :, pl.ds(0, LANES)], x_front, behind["gx"]),
        (theta_ref.at[pl.ds(rows - HALO, HALO)], y_back, ahead["gy"]),
        (theta_ref.at[pl.ds(0, HALO)], y_front, behind["gy"]),
    ]
    copies = []
    for number, (source, place, device) in enumerate(sends):
        copy = pltpu.make_async_remote_copy(
            src_ref=source,
            dst_ref=place,
            send_sem=send_sem.at[number],
            recv_sem=recv_sem.at[number],
            device_id=device,
            device_id_type=MESH,
        )
        copy.start()
        copies.append(copy)
    own = pltpu.make_async_copy(seg_ref.at[me], out_ref.at[me], own_sem)
    own.start()
    own.wait()
    for copy in copies:
        copy.wait()


def exchange_faces(segments, theta):
    sizes = tuple(lax.axis_size(axis) for axis in ("gx", "gy", "gz"))
    rows, depth, cells = theta.shape
    shapes = [
        segments.shape,
        (rows, depth, LANES),
        (rows, depth, LANES),
        (HALO, depth, cells),
        (HALO, depth, cells),
        (rows, HALO, cells),
        (rows, HALO, cells),
    ]
    count = sizes[0] - 1 + 6
    return pl.pallas_call(
        functools.partial(faces_kernel, sizes),
        out_shape=[jax.ShapeDtypeStruct(shape, jnp.float32) for shape in shapes],
        in_specs=whole_vmem(2),
        out_specs=whole_vmem(7),
        scratch_shapes=[
            pltpu.SemaphoreType.DMA((count,)),
            pltpu.SemaphoreType.DMA((count,)),
            pltpu.SemaphoreType.DMA,
        ],
        compiler_params=pltpu.CompilerParams(collective_id=1, has_side_effects=True),
        name="faces",
    )(segments, theta)


CHUNK = 256


def section_kernel(
    offset_ref, length_ref, seg_ref, x_back, x_front, y_back, y_front, z_back, z_front,
    theta_ref, sum_ref, index_ref, weight_ref, theta_out, sum_out,
    gathered, pieces, carried, deep, position, top_weight, rest_weight,
):
    me = lax.axis_index("gx")
    rows, depth, cells = theta_ref.shape
    blocks, span, lines, _ = seg_ref.shape
    taps = index_ref.shape[0]
    total = blocks * lines
    for block in range(blocks):
        gathered[0:span, block * lines : (block + 1) * lines, :] = seg_ref[block]
    top, rest = split(gathered[0:span])
    pieces[0:span, 0:total, :] = top
    pieces[0:span, total:, :] = rest
    pieces[span] = jnp.zeros(pieces.shape[1:], pieces.dtype)

    columns = pl.ds(pl.multiple_of(me * cells, LANES), cells)
    index = index_ref[:, columns]
    weight = jnp.where(index < length_ref[me], weight_ref[:, columns], 0.0)
    live = index < length_ref[me]
    merged = jnp.zeros_like(weight)
    for tap in range(taps):
        merged = merged + jnp.where(index == index[tap : tap + 1], weight[tap : tap + 1], 0.0)
    high, low = split(merged)
    top_weight[...] = high.astype(jnp.float32)
    rest_weight[...] = low.astype(jnp.float32)
    begin = offset_ref[me] - length_ref[blocks + me] * LANES
    place = index + begin
    position[...] = jnp.where(live, place, -1)
    bounds = []
    for chunk in range(cells // CHUNK):
        part = slice(chunk * CHUNK, (chunk + 1) * CHUNK)
        seen = live[:, part]
        least = jnp.min(jnp.where(seen, place[:, part], span * LANES))
        most = jnp.max(jnp.where(seen, place[:, part], -1))
        bounds.append((least // LANES, (most + LANES) // LANES))

    counter = lax.broadcasted_iota(jnp.int32, (2 * LANES, CHUNK), 0).astype(jnp.float32).astype(jnp.bfloat16)
    for chunk in range(cells // CHUNK):
        part = slice(chunk * CHUNK, (chunk + 1) * CHUNK)
        least, end = bounds[chunk]

        def tile(step, acc):
            slab = least + 2 * step
            near = position[:, part] - slab * LANES
            near = jnp.clip(near, -1, 2 * LANES).astype(jnp.float32)
            near = near.astype(jnp.bfloat16)
            tops = top_weight[:, part].astype(jnp.bfloat16)
            rests = rest_weight[:, part].astype(jnp.bfloat16)
            matrix_top = jnp.zeros((2 * LANES, CHUNK), jnp.bfloat16)
            matrix_rest = jnp.zeros((2 * LANES, CHUNK), jnp.bfloat16)
            for tap in range(taps):
                hit = counter == near[tap : tap + 1]
                matrix_top = jnp.where(hit, tops[tap : tap + 1], matrix_top)
                matrix_rest = jnp.where(hit, rests[tap : tap + 1], matrix_rest)
            values = jnp.concatenate([pieces[slab], pieces[slab + 1]], axis=1)
            first = jnp.dot(values, matrix_top, preferred_element_type=jnp.float32)
            second = jnp.dot(values[:total], matrix_rest, preferred_element_type=jnp.float32)
            return acc + (first[:total] + (first[total:] + second))

        result = lax.fori_loop(
            0, (end - least + 1) // 2, tile, jnp.zeros((total, CHUNK), jnp.float32)
        )
        own = lines // (3 * depth)
        for block in range(blocks):
            for comp in range(3):
                for row in range(own):
                    at = block * lines + (comp * own + row) * depth
                    carried[comp, block * own + row, :, part] = result[at : at + depth]

    deep[:, 0:HALO, :] = z_back[...]
    deep[:, HALO : HALO + depth, :] = theta_ref[...]
    deep[:, HALO + depth :, :] = z_front[...]

    def line(row):
        if row < 0:
            return y_back[HALO + row]
        if row >= rows:
            return y_front[row - rows]
        return theta_ref[row]

    for row in range(rows):
        center = theta_ref[row]
        wide = jnp.concatenate([x_back[row], center, x_front[row]], axis=1)
        width = wide.shape[1]
        grads = [None, None, None]
        laplace = 3.0 * center_coeff * center
        for reach in range(1, 5):
            pairs = [
                (
                    pltpu.roll(wide, width - reach, 1)[:, LANES : LANES + cells],
                    pltpu.roll(wide, reach, 1)[:, LANES : LANES + cells],
                ),
                (line(row + reach), line(row - reach)),
                (deep[row, HALO + reach : HALO + reach + depth], deep[row, HALO - reach : HALO - reach + depth]),
            ]
            joined = None
            for axis, (ahead, behind) in enumerate(pairs):
                term = first_coeffs[reach - 1] * (ahead - behind)
                grads[axis] = term if grads[axis] is None else grads[axis] + term
                both = ahead + behind
                joined = both if joined is None else joined + both
            laplace = laplace + second_coeffs[reach - 1] * joined
        moved = carried[0, row] * grads[0] + carried[1, row] * grads[1] + carried[2, row] * grads[2]
        change = diffusivity * laplace - moved
        after = section_keep * sum_ref[row] + time_step * change
        sum_out[row] = after
        theta_out[row] = center + section_gain * after


def finish(seg_offset, seg_table, segments, halos, theta, section_sum, stencil_index, stencil_weight):
    blocks, span, lines, _ = segments.shape
    rows, depth, cells = theta.shape
    taps = stencil_index.shape[0]
    return pl.pallas_call(
        section_kernel,
        out_shape=[jax.ShapeDtypeStruct(theta.shape, jnp.float32)] * 2,
        in_specs=[pl.BlockSpec(memory_space=pltpu.SMEM)] * 2 + whole_vmem(11),
        out_specs=whole_vmem(2),
        scratch_shapes=[
            VMEM((span, blocks * lines, LANES), jnp.float32),
            VMEM((span + 1, 2 * blocks * lines, LANES), jnp.bfloat16),
            VMEM((3, rows, depth, cells), jnp.float32),
            VMEM((rows, depth + 2 * HALO, cells), jnp.float32),
            VMEM((taps, cells), jnp.int32),
            VMEM((taps, cells), jnp.float32),
            VMEM((taps, cells), jnp.float32),
        ],
        name="section",
    )(seg_offset, seg_table, segments, *halos, theta, section_sum, stencil_index, stencil_weight)


def body(spectrum, theta, section_sum, seg_offset, seg_length, stencil_index, stencil_weight):
    modes = exchange_modes(spectrum)
    modes = modes.reshape((-1,) + modes.shape[2:])
    segments = transform_lines(seg_offset, modes)
    segments, *halos = exchange_faces(segments, theta)
    far = 2 * modes.shape[0]
    start = jnp.minimum(seg_offset // LANES, far - segments.shape[1])
    return tuple(
        finish(
            seg_offset, jnp.concatenate([seg_length, start]), segments, halos, theta, section_sum,
            stencil_index, stencil_weight,
        )
    )


def solution(mesh):
    placed = (
        P(None, None, ("gy", "gx"), None, "gz"),
        P("gy", "gz", "gx"),
        P("gy", "gz", "gx"),
        P(),
        P(),
        P(),
        P(),
    )
    return jax.shard_map(
        body,
        mesh=mesh,
        in_specs=placed,
        out_specs=(P("gy", "gz", "gx"), P("gy", "gz", "gx")),
        check_vma=False,
    )
```

```python
import functools
import math

import jax
import jax.numpy as jnp
import numpy as np
from jax import lax
from jax.experimental import pallas as pl
from jax.experimental.pallas import tpu as pltpu
from jax.sharding import PartitionSpec as P

MESH = pl.DeviceIdType.MESH
VMEM = pltpu.VMEM
LANES = 128
HALO = 4

first_coeffs = (0.8, -0.2, 4.0 / 105.0, -1.0 / 280.0)
second_coeffs = (1.6, -0.2, 8.0 / 315.0, -1.0 / 560.0)
center_coeff = -205.0 / 72.0
diffusivity = 0.15
time_step = 0.4
section_keep = -5.0 / 9.0
section_gain = 15.0 / 16.0


def whole_vmem(count):
    return [pl.BlockSpec(memory_space=VMEM)] * count


def rotate(value, turn):
    re, im = value
    cosine, sine = math.cos(2 * math.pi * turn), math.sin(2 * math.pi * turn)
    quarter = turn * 4 % 4
    if quarter == 0:
        return re, im
    if quarter == 1:
        return -im, re
    if quarter == 2:
        return -re, -im
    if quarter == 3:
        return im, -re
    return re * cosine - im * sine, re * sine + im * cosine


def fft(values):
    count = len(values)
    if count == 1:
        return values
    even = fft(values[0::2])
    odd = fft(values[1::2])
    low, high = [], []
    for x in range(count // 2):
        re, im = rotate(odd[x], x / count)
        low.append((even[x][0] + re, even[x][1] + im))
        high.append((even[x][0] - re, even[x][1] - im))
    return low + high


def split(value):
    top = value.astype(jnp.bfloat16)
    return top, (value - top.astype(jnp.float32)).astype(jnp.bfloat16)


def section_kernel(
    sizes, span,
    offset_ref, length_ref, spec_ref, theta_ref, sum_ref, index_ref, weight_ref, twist_ref, last_ref,
    theta_out, sum_out,
    modes_send, modes_recv, mixed, velocity, seg_send, seg_recv, matrix_top, matrix_rest, gathered, values,
    grads, laplace, deep, x_back, x_front, y_back, y_front, z_back, z_front,
    modes_sems, seg_sems, face_sems,
):
    gx, gy, gz = sizes
    here = {axis: lax.axis_index(axis) for axis in ("gx", "gy", "gz")}
    counts = dict(gx=gx, gy=gy, gz=gz)
    ahead = {axis: {axis: lax.rem(here[axis] + 1, counts[axis])} for axis in here}
    behind = {axis: {axis: lax.rem(here[axis] + counts[axis] - 1, counts[axis])} for axis in here}
    rows, depth, cells = theta_ref.shape
    _, _, own_rows, all_depth, modes = spec_ref.shape
    local_slabs = modes // LANES
    group = own_rows * depth
    slabs = gz * local_slabs
    near = 2 * slabs
    far = 2 * slabs
    taps = index_ref.shape[0]

    barrier = pltpu.get_barrier_semaphore()
    targets = [{"gx": lax.rem(here["gx"] + step, gx)} for step in range(1, gx)]
    targets += [{"gz": lax.rem(here["gz"] + step, gz)} for step in range(1, gz)]
    targets += [ahead["gy"], behind["gy"]]
    for target in targets:
        pl.semaphore_signal(barrier, inc=1, device_id=target, device_id_type=MESH)

    for comp in range(3):
        for slab in range(local_slabs):
            for part in range(2):
                for row in range(own_rows):
                    held = spec_ref[comp, part, row, :, slab * LANES : (slab + 1) * LANES]
                    at = part * group + row * depth
                    for peer in range(gz):
                        modes_send[comp, peer, slab, at : at + depth, :] = held[
                            peer * depth : (peer + 1) * depth
                        ]
    pl.semaphore_wait(barrier, len(targets))

    def modes_copy(comp, step):
        target = lax.rem(here["gz"] + step, gz)
        return pltpu.make_async_remote_copy(
            src_ref=modes_send.at[comp, target],
            dst_ref=modes_recv.at[comp, here["gz"]],
            send_sem=modes_sems.at[0, comp, step - 1],
            recv_sem=modes_sems.at[1, comp, step - 1],
            device_id={"gz": target},
            device_id_type=MESH,
        )

    def seg_copy(comp, step):
        target = lax.rem(here["gx"] + step, gx)
        return pltpu.make_async_remote_copy(
            src_ref=seg_send.at[comp, target],
            dst_ref=seg_recv.at[comp, here["gx"]],
            send_sem=seg_sems.at[0, comp, step - 1],
            recv_sem=seg_sems.at[1, comp, step - 1],
            device_id={"gx": target},
            device_id_type=MESH,
        )

    faces = [
        pltpu.make_async_remote_copy(
            src_ref=source,
            dst_ref=place,
            send_sem=face_sems.at[0, number],
            recv_sem=face_sems.at[1, number],
            device_id=device,
            device_id_type=MESH,
        )
        for number, (source, place, device) in enumerate(
            [
                (theta_ref.at[:, :, pl.ds(cells - LANES, LANES)], x_back, ahead["gx"]),
                (theta_ref.at[:, :, pl.ds(0, LANES)], x_front, behind["gx"]),
                (theta_ref.at[pl.ds(rows - HALO, HALO)], y_back, ahead["gy"]),
                (theta_ref.at[pl.ds(0, HALO)], y_front, behind["gy"]),
                (theta_ref.at[:, pl.ds(depth - HALO, HALO), :], z_back, ahead["gz"]),
                (theta_ref.at[:, pl.ds(0, HALO), :], z_front, behind["gz"]),
            ]
        )
    ]
    for comp in range(3):
        for step in range(1, gz):
            modes_copy(comp, step).start()
    for face in faces:
        face.start()
    for comp in range(3):
        modes_recv[comp, here["gz"]] = modes_send[comp, here["gz"]]

    me = here["gx"]
    live_count = length_ref[me]
    begin = offset_ref[me] - jnp.minimum(offset_ref[me] // LANES, far - span) * LANES
    counter = lax.broadcasted_iota(jnp.int32, (LANES, LANES), 0).astype(jnp.float32).astype(jnp.bfloat16)

    def spread(row):
        one = jnp.broadcast_to(row, (16, LANES)).astype(jnp.bfloat16)
        return jnp.concatenate([one] * (LANES // 16), axis=0)

    def build(chunk, carry):
        columns = pl.ds(pl.multiple_of(me * cells + chunk * LANES, LANES), LANES)
        index = index_ref[:, columns]
        live = index < live_count
        weight = jnp.where(live, weight_ref[:, columns], 0.0)
        merged = jnp.zeros_like(weight)
        for tap in range(taps):
            merged = merged + jnp.where(index == index[tap : tap + 1], weight[tap : tap + 1], 0.0)
        high, low = split(merged)
        high, low = high.astype(jnp.float32), low.astype(jnp.float32)
        place = jnp.where(live, index + begin, -1)
        tops = [spread(high[tap : tap + 1]) for tap in range(taps)]
        rests = [spread(low[tap : tap + 1]) for tap in range(taps)]

        def slab_of(slab, inner):
            close = jnp.clip(place - slab * LANES, -1, LANES).astype(jnp.float32)
            top = jnp.zeros((LANES, LANES), jnp.bfloat16)
            rest = jnp.zeros((LANES, LANES), jnp.bfloat16)
            for tap in range(taps):
                hit = counter == spread(close[tap : tap + 1])
                top = jnp.where(hit, tops[tap], top)
                rest = jnp.where(hit, rests[tap], rest)
            at = pl.ds(pl.multiple_of(slab * LANES, LANES), LANES)
            matrix_top[chunk, at, :] = top
            matrix_rest[chunk, at, :] = rest
            return inner

        return lax.fori_loop(0, span, slab_of, carry)

    lax.fori_loop(0, cells // LANES, build, 0)

    last_both = last_ref[...]
    last_top = last_both[:far]
    dims = (((1,), (1,)), ((), ()))

    def twisted(line):
        re, im = mixed[:, line, :], mixed[:, group + line, :]
        pieces = []
        for quarter in range(LANES // near):
            part = slice(quarter * near, (quarter + 1) * near)
            cosine, sine = twist_ref[0, part, :], twist_ref[1, part, :]
            pieces.append(jnp.concatenate([re * cosine - im * sine, re * sine + im * cosine], axis=1))
        return jnp.concatenate(pieces, axis=0)

    def transform(comp, carry):
        for step in range(1, gz):
            modes_copy(comp, step).wait()

        def arrived(k):
            held = modes_recv[comp, k // local_slabs, k % local_slabs]
            return held[:group], held[group:]

        for parity in range(2):
            mixes = fft([rotate(arrived(k), parity * k / near) for k in range(slabs)])
            for x in range(slabs):
                mixed[2 * x + parity, 0:group, :] = mixes[x][0]
                mixed[2 * x + parity, group:, :] = mixes[x][1]
        for pair in range(group // 2):
            turned = jnp.concatenate([twisted(2 * pair), twisted(2 * pair + 1)], axis=0)
            top, rest = split(turned)
            first = lax.dot_general(last_both, top, dims, preferred_element_type=jnp.float32)
            second = lax.dot_general(last_top, rest, dims, preferred_element_type=jnp.float32)
            total = first[:far] + (first[far:] + second)
            velocity[:, 2 * pair, :] = total[:, :LANES]
            velocity[:, 2 * pair + 1, :] = total[:, LANES:]
        for block in range(gx):
            start = jnp.minimum(offset_ref[block] // LANES, far - span)
            seg_send[comp, block] = velocity[pl.ds(start, span)]
        for step in range(1, gx):
            seg_copy(comp, step).start()
        seg_recv[comp, me] = seg_send[comp, me]
        return carry

    lax.fori_loop(0, 3, transform, 0)

    for face in faces[:4]:
        face.wait()

    def line(row):
        if row < 0:
            return y_back[HALO + row]
        if row >= rows:
            return y_front[row - rows]
        return theta_ref[row]

    for row in range(rows):
        at = slice(row * depth, (row + 1) * depth)
        center = theta_ref[row]
        wide = jnp.concatenate([x_back[row], center, x_front[row]], axis=1)
        width = wide.shape[1]
        grad_x = jnp.zeros_like(center)
        grad_y = jnp.zeros_like(center)
        partial = 3.0 * center_coeff * center
        for reach in range(1, 5):
            ahead_x = pltpu.roll(wide, width - reach, 1)[:, LANES : LANES + cells]
            behind_x = pltpu.roll(wide, reach, 1)[:, LANES : LANES + cells]
            ahead_y, behind_y = line(row + reach), line(row - reach)
            grad_x = grad_x + first_coeffs[reach - 1] * (ahead_x - behind_x)
            grad_y = grad_y + first_coeffs[reach - 1] * (ahead_y - behind_y)
            partial = partial + second_coeffs[reach - 1] * (ahead_x + behind_x + ahead_y + behind_y)
        grads[0, at, :] = grad_x
        grads[1, at, :] = grad_y
        laplace[at, :] = partial
    for face in faces[4:]:
        face.wait()
    deep[:, 0:HALO, :] = z_back[...]
    deep[:, HALO : HALO + depth, :] = theta_ref[...]
    deep[:, HALO + depth :, :] = z_front[...]
    for row in range(rows):
        at = slice(row * depth, (row + 1) * depth)
        grad_z = jnp.zeros((depth, cells), jnp.float32)
        partial = laplace[at, :]
        for reach in range(1, 5):
            ahead_z = deep[row, HALO + reach : HALO + reach + depth]
            behind_z = deep[row, HALO - reach : HALO - reach + depth]
            grad_z = grad_z + first_coeffs[reach - 1] * (ahead_z - behind_z)
            partial = partial + second_coeffs[reach - 1] * (ahead_z + behind_z)
        grads[2, at, :] = grad_z
        change = diffusivity * partial
        laplace[at, :] = section_keep * sum_ref[row] + time_step * change

    for comp in range(3):
        for step in range(1, gx):
            seg_copy(comp, step).wait()
    lines = gx * group
    for comp in range(3):
        for block in range(gx):
            at = (comp * gx + block) * group
            for slab in range(span):
                gathered[at : at + group, slab * LANES : (slab + 1) * LANES] = seg_recv[comp, block, slab]
    total = 3 * lines
    top, rest = split(gathered[...])
    values[0:total, :] = top
    values[total:, :] = rest

    def combine(pair, carry):
        top = jnp.concatenate([matrix_top[2 * pair], matrix_top[2 * pair + 1]], axis=1)
        rest = jnp.concatenate([matrix_rest[2 * pair], matrix_rest[2 * pair + 1]], axis=1)
        first = jnp.dot(values[...], top, preferred_element_type=jnp.float32)
        second = jnp.dot(values[0:total, :], rest, preferred_element_type=jnp.float32)
        moved = first[:total] + (first[total:] + second)
        columns = pl.ds(pl.multiple_of(pair * 2 * LANES, 2 * LANES), 2 * LANES)
        carried = None
        for comp in range(3):
            term = moved[comp * lines : (comp + 1) * lines] * grads[comp, :, columns]
            carried = term if carried is None else carried + term
        after = laplace[:, columns] - time_step * carried
        for row in range(rows):
            piece = after[row * depth : (row + 1) * depth]
            sum_out[row, :, columns] = piece
            theta_out[row, :, columns] = theta_ref[row, :, columns] + section_gain * piece
        return carry

    lax.fori_loop(0, cells // (2 * LANES), combine, 0)


def body(spectrum, theta, section_sum, seg_offset, seg_length, stencil_index, stencil_weight):
    sizes = tuple(lax.axis_size(axis) for axis in ("gx", "gy", "gz"))
    gx, _, gz = sizes
    _, _, own_rows, all_depth, modes = spectrum.shape
    rows, depth, cells = theta.shape
    group = own_rows * depth
    slabs = gz * modes // LANES
    length = 2 * slabs * LANES
    far = length // LANES
    span = min(3 * length // (2 * gx) // LANES + 1, far)
    k = np.arange(LANES)
    turn = 2 * np.pi * (np.outer(k, k) % length) / length
    twist = np.stack([np.cos(turn), np.sin(turn)]).astype(np.float32)
    turn = 2 * np.pi * (np.outer(np.arange(far), k) % far) / far
    last = np.concatenate([np.cos(turn), -np.sin(turn)], axis=1).astype(np.float32)
    top = last.astype(jnp.bfloat16)
    rest = (last - top.astype(np.float32)).astype(jnp.bfloat16)
    modes_shape = (3, gz, modes // LANES, 2 * group, LANES)
    seg_shape = (3, gx, span, group, LANES)
    lines = gx * group
    single = jnp.float32
    return tuple(
        pl.pallas_call(
            functools.partial(section_kernel, sizes, span),
            out_shape=[jax.ShapeDtypeStruct(theta.shape, single)] * 2,
            in_specs=[pl.BlockSpec(memory_space=pltpu.SMEM)] * 2 + whole_vmem(7),
            out_specs=whole_vmem(2),
            scratch_shapes=[
                VMEM(modes_shape, single),
                VMEM(modes_shape, single),
                VMEM((2 * slabs, 2 * group, LANES), single),
                VMEM((far, group, LANES), single),
                VMEM(seg_shape, single),
                VMEM(seg_shape, single),
                VMEM((cells // LANES, span * LANES, LANES), jnp.bfloat16),
                VMEM((cells // LANES, span * LANES, LANES), jnp.bfloat16),
                VMEM((3 * lines, span * LANES), single),
                VMEM((6 * lines, span * LANES), jnp.bfloat16),
                VMEM((3, rows * depth, cells), single),
                VMEM((rows * depth, cells), single),
                VMEM((rows, depth + 2 * HALO, cells), single),
                VMEM((rows, depth, LANES), single),
                VMEM((rows, depth, LANES), single),
                VMEM((HALO, depth, cells), single),
                VMEM((HALO, depth, cells), single),
                VMEM((rows, HALO, cells), single),
                VMEM((rows, HALO, cells), single),
                pltpu.SemaphoreType.DMA((2, 3, gz - 1)),
                pltpu.SemaphoreType.DMA((2, 3, gx - 1)),
                pltpu.SemaphoreType.DMA((2, 6)),
            ],
            compiler_params=pltpu.CompilerParams(
                collective_id=0, has_side_effects=True, vmem_limit_bytes=60 * 1024 * 1024
            ),
            name="section",
        )(
            seg_offset, seg_length, spectrum, theta, section_sum, stencil_index, stencil_weight,
            jnp.asarray(twist), jnp.asarray(np.concatenate([top, rest], axis=0)),
        )
    )


def solution(mesh):
    placed = (
        P(None, None, ("gy", "gx"), None, "gz"),
        P("gy", "gz", "gx"),
        P("gy", "gz", "gx"),
        P(),
        P(),
        P(),
        P(),
    )
    return jax.shard_map(
        body,
        mesh=mesh,
        in_specs=placed,
        out_specs=(P("gy", "gz", "gx"), P("gy", "gz", "gx")),
        check_vma=False,
    )
```
